32 devices in a mesh: rep: 2 (over x), dp: 16 (over y, z, core).
Axes of the slice: x: 2, y: 2, z: 4, core: 2. Of those that a mesh axis runs over, the one named last changes fastest.
Arguments:
- x: bfloat16 [32, 2048, 896], P(('rep', 'dp')), parts along dimension 0
- dy: bfloat16 [32, 2048, 896], P(('rep', 'dp')), parts along dimension 0
- w_gate: bfloat16 [2, 896, 2560], replicated
- w_up: bfloat16 [2, 896, 2560], replicated
- w_down: bfloat16 [2, 2560, 896], replicated
- m_w_gate: float32 [2, 896, 2560], P(None, 'dp')
- m_w_up: float32 [2, 896, 2560], P(None, 'dp')
- m_w_down: float32 [2, 2560, 896], P(None, 'dp')
- v_w_gate: float32 [2, 896, 2560], P(None, 'dp')
- v_w_up: float32 [2, 896, 2560], P(None, 'dp')
- v_w_down: float32 [2, 2560, 896], P(None, 'dp')
Outputs:
- output 1: bfloat16 [4, 896, 2560], P('rep'), parts along dimension 0
- output 2: bfloat16 [4, 896, 2560], P('rep'), parts along dimension 0
- output 3: bfloat16 [4, 2560, 896], P('rep'), parts along dimension 0
- output 4: float32 [4, 896, 2560], P('rep', 'dp'), parts along dimension 0
- output 5: float32 [4, 896, 2560], P('rep', 'dp'), parts along dimension 0
- output 6: float32 [4, 2560, 896], P('rep', 'dp'), parts along dimension 0
- output 7: float32 [4, 896, 2560], P('rep', 'dp'), parts along dimension 0
- output 8: float32 [4, 896, 2560], P('rep', 'dp'), parts along dimension 0
- output 9: float32 [4, 2560, 896], P('rep', 'dp'), parts along dimension 0
There are 2 independent parts. The reference program is written for one: setup_inputs(seed, part) draws one part's arguments, and reference() takes and returns one part's arrays. A program takes and returns all parts, laid end to end along the dimension named above; an argument that names none is the same for every part.
All inputs are finite; a program needn't handle non-finite values.
Results may differ from the reference program's by a relative error of at most 0.022.
Values are sent between devices in bfloat16 or wider.
A program may use at most 2 GiB of HBM per device.

```python
import jax
import jax.numpy as jnp
from jax import lax

SEQUENCES = 16
TOKENS = 2048
D = 896
FF = 2560
LAYERS = 2
NAMES = ("w_gate", "w_up", "w_down")
SHAPES = {"w_gate": (LAYERS, D, FF), "w_up": (LAYERS, D, FF), "w_down": (LAYERS, FF, D)}


def bump(key, n, height):
    away = (jnp.arange(n, dtype=jnp.int32) - jax.random.randint(key, (), 0, n, jnp.int32)) % n
    return jnp.where(away < n // 8, height, 1.0)


def together(key, own, strength):
    shared = jax.random.normal(key, own.shape[1:], jnp.float32)
    return (own + strength * shared) * lax.rsqrt(1 + strength * strength)


def setup_inputs(seed: int = 0, part: int = 0) -> dict:
    kx, kdy, ka, kb, kz, kf, kh, kl, *keys = jax.random.split(jax.random.key(seed), 8 + 3 * len(NAMES))
    kx, kdy, ka, kb = (jax.random.fold_in(k, part) for k in (kx, kdy, ka, kb))
    kw, km, kv = (keys[i::3] for i in range(3))
    shape = (SEQUENCES, TOKENS, D)
    much_x, much_dy = jax.random.uniform(kz, (2,), jnp.float32, 0.0, 1.0)
    loud = 2.0 ** jax.random.uniform(jax.random.fold_in(kz, 1), (), jnp.float32, -1.0, 2.0)
    layers = 2.0 ** jax.random.uniform(kl, (LAYERS, 1, 1), jnp.float32, -1.0, 1.0)
    x = together(ka, jax.random.normal(kx, shape, jnp.float32), much_x) * bump(kf, D, 4.0)
    dy = together(kb, jax.random.normal(kdy, shape, jnp.float32), much_dy)
    drawn = {"x": x.astype(jnp.bfloat16), "dy": (loud * dy * (SEQUENCES * TOKENS) ** -0.5).astype(jnp.bfloat16)}
    for key, name in zip(kw, NAMES, strict=True):
        w = jax.random.normal(key, SHAPES[name], jnp.float32) * SHAPES[name][1] ** -0.5
        drawn[name] = (w * {"w_gate": 1.0, "w_up": bump(kh, FF, 4.0), "w_down": layers}[name]).astype(jnp.bfloat16)
    for key, name in zip(km, NAMES, strict=True):
        drawn[f"m_{name}"] = 0.1 * jax.random.normal(key, SHAPES[name], jnp.float32)
    for key, name in zip(kv, NAMES, strict=True):
        drawn[f"v_{name}"] = jax.random.uniform(key, SHAPES[name], jnp.float32, 0.005, 0.015)
    return drawn


def matmul(a, w):
    return jnp.dot(a, w, preferred_element_type=jnp.float32).astype(jnp.bfloat16)


def normed(h):
    wide = h.astype(jnp.float32)
    scale = lax.rsqrt(jnp.mean(wide**2, -1, keepdims=True) + 1e-6)
    return (wide * scale).astype(jnp.bfloat16)


def layer(h, w):
    a = normed(h)
    gate = jnp.dot(a, w["w_gate"], preferred_element_type=jnp.float32)
    up = jnp.dot(a, w["w_up"], preferred_element_type=jnp.float32)
    return h + matmul((jax.nn.silu(gate) * up).astype(jnp.bfloat16), w["w_down"])


def adamw(w, m, v, g):
    m = 0.9 * m + 0.1 * g
    v = 0.95 * v + 0.05 * g * g
    step = m * lax.rsqrt(v + 1e-8) + 0.1 * w
    return (w - 0.02 * step).astype(jnp.bfloat16), m, v


def stack(weights, h):
    return lax.scan(lambda h, w: (layer(h, w), None), h, weights)[0]


def reference(x, dy, w_gate, w_up, w_down, m_w_gate, m_w_up, m_w_down, v_w_gate, v_w_up, v_w_down):
    weights = dict(zip(NAMES, (w_gate, w_up, w_down), strict=True))

    def take(so_far, sequence):
        h, by_y = sequence
        _, back = jax.vjp(lambda w: stack(w, h), weights)
        return jax.tree.map(lambda total, term: total + term.astype(jnp.float32), so_far, back(by_y)[0]), None

    none_yet = {name: jnp.zeros(w.shape, jnp.float32) for name, w in weights.items()}
    by_weights, _ = lax.scan(take, none_yet, (x, dy))
    gradients = [by_weights[name].astype(jnp.bfloat16).astype(jnp.float32) for name in NAMES]
    new = [
        adamw(w.astype(jnp.float32), m, v, g)
        for w, m, v, g in zip((w_gate, w_up, w_down), (m_w_gate, m_w_up, m_w_down), (v_w_gate, v_w_up, v_w_down), gradients, strict=True)
    ]
    return tuple(one[which] for which in range(3) for one in new)
```

```python
import functools

import jax
import jax.numpy as jnp
from jax import lax
from jax.experimental import pallas as pl
from jax.experimental.pallas import tpu as pltpu
from jax.sharding import PartitionSpec as P

F32, BF16 = jnp.float32, jnp.bfloat16


def dot(a, b, contract):
    return lax.dot_general(a, b, (contract, ((), ())), preferred_element_type=F32)


def nn(a, b):
    return dot(a, b, ((1,), (0,)))


def nt(a, b):
    return dot(a, b, ((1,), (1,)))


def tn(a, b):
    return dot(a, b, ((0,), (0,)))


def adamw(w, m, v, g):
    m = 0.9 * m + 0.1 * g
    v = 0.95 * v + 0.05 * g * g
    step = m * lax.rsqrt(v + 1e-8) + 0.1 * w
    return (w - 0.02 * step).astype(BF16), m, v


def normed(h):
    wide = h.astype(F32)
    scale = lax.rsqrt(jnp.mean(wide**2, -1, keepdims=True) + 1e-6)
    return (wide * scale).astype(BF16)


def normed_back(h, da):
    wide, da = h.astype(F32), da.astype(F32)
    scale = lax.rsqrt(jnp.mean(wide**2, -1, keepdims=True) + 1e-6)
    inner = jnp.mean(wide * da, -1, keepdims=True)
    return (da * scale - wide * (scale * scale * scale * inner)).astype(BF16)


def hidden(a, wg, wu):
    gate, up = nn(a, wg), nn(a, wu)
    return gate, up, (jax.nn.silu(gate) * up).astype(BF16)


def hidden_back(gate, up, dact):
    s = jax.nn.sigmoid(gate)
    dact = dact.astype(F32)
    dup = dact * gate * s
    dgate = dact * up * (s * (1.0 + gate * (1.0 - s)))
    return dgate.astype(BF16), dup.astype(BF16)


MESH = pl.DeviceIdType.MESH


def ring_kernel(order, shapes, *refs):
    n = len(order)
    take = iter(refs)
    g = [next(take) for _ in range(n)]
    w, m, v = ([next(take) for _ in range(3)] for _ in range(3))
    w_new, m_new, v_new = ([next(take) for _ in range(3)] for _ in range(3))
    own, sib, rec, wv, mv, vv = ([next(take) for _ in range(n)] for _ in range(6))
    (own_sem, sib_send, sib_recv, rs_send, rs_recv, ag_send, ag_recv, pass_send, pass_recv, load_sem, store_sem) = take

    me = lax.axis_index("dp")
    core, chip = me % 2, me // 2
    far = chip // 4
    place = chip * (1 - far) + far * (11 - chip)
    way = 1 - 2 * core

    def chip_at(p):
        p = (p + 16) % 8
        half = p // 4
        return p * (1 - half) + half * (11 - p)

    after = 2 * chip_at(place + way) + core
    before = 2 * chip_at(place - way) + core
    twin = me + way

    barrier = pltpu.get_barrier_semaphore()
    for other in (after, before, twin):
        pl.semaphore_signal(barrier, inc=1, device_id={"dp": other}, device_id_type=MESH)

    def own_copy(k, j):
        t = chip_at(place - way * (1 + j))
        return pltpu.make_async_copy(g[k].at[t, core], own[k].at[j], own_sem.at[k, j])

    def sib_copy(k, j):
        t = chip_at(place + way * (1 + j))
        return pltpu.make_async_remote_copy(
            g[k].at[t, 1 - core], sib[k].at[j], sib_send.at[k, j], sib_recv.at[k, j], {"dp": twin}, MESH
        )

    def ring_copy(k, j):
        return pltpu.make_async_remote_copy(
            own[k].at[j], rec[k].at[j], rs_send.at[k, j], rs_recv.at[k, j], {"dp": after}, MESH
        )

    def loads(k):
        name, layer = order[k]
        return (
            pltpu.make_async_copy(w[name].at[layer, me], wv[k], load_sem.at[k, 0]),
            pltpu.make_async_copy(m[name].at[layer], mv[k], load_sem.at[k, 1]),
            pltpu.make_async_copy(v[name].at[layer], vv[k], load_sem.at[k, 2]),
        )

    def stores(k):
        name, layer = order[k]
        return (
            pltpu.make_async_copy(wv[k], w_new[name].at[layer, me], store_sem.at[k, 0]),
            pltpu.make_async_copy(mv[k], m_new[name].at[layer], store_sem.at[k, 1]),
            pltpu.make_async_copy(vv[k], v_new[name].at[layer], store_sem.at[k, 2]),
        )

    def gather_copy(k, j, source):
        name, layer = order[k]
        at = 2 * chip_at(place - way * j) + core
        there = w_new[name].at[layer, at]
        source = there if source is None else source
        return pltpu.make_async_remote_copy(source, there, ag_send.at[k, j], ag_recv.at[k, j], {"dp": after}, MESH)

    def twin_copy(k, j, source):
        name, layer = order[k]
        at = 2 * chip_at(place - way * j) + core
        there = w_new[name].at[layer, at]
        source = there if source is None else source
        return pltpu.make_async_remote_copy(source, there, pass_send.at[k, j], pass_recv.at[k, j], {"dp": twin}, MESH)

    def over_columns(k, body):
        rows, columns = shapes[order[k][0]]
        wide = 256 if columns % 256 == 0 and rows < 100 else 128

        def piece(c, carry):
            body(pl.ds(pl.multiple_of(c * wide, wide), wide))
            return carry

        lax.fori_loop(0, columns // wide, piece, 0)

    @pl.loop(0, 8)
    def _(j):
        for k in range(n):
            own_copy(k, j).start()

    pl.semaphore_wait(barrier, 3)

    @pl.loop(0, 8)
    def _(j):
        for k in range(n):
            sib_copy(k, j).start()

    for k in range(n):
        for copy in loads(k):
            copy.start()

    def first(k):
        own_copy(k, 0).wait()
        sib_copy(k, 0).wait_recv()

        def add(at):
            own[k][0, :, at] = (own[k][0, :, at].astype(F32) + sib[k][0, :, at].astype(F32)).astype(BF16)

        over_columns(k, add)
        ring_copy(k, 0).start()

    for k in range(n):
        first(k)

    @pl.loop(1, 7)
    def _(j):
        for k in range(n):
            own_copy(k, j).wait()
            sib_copy(k, j).wait_recv()
            ring_copy(k, j - 1).wait_recv()

            def add(at, k=k):
                total = own[k][j, :, at].astype(F32) + sib[k][j, :, at].astype(F32) + rec[k][j - 1, :, at].astype(F32)
                own[k][j, :, at] = total.astype(BF16)

            over_columns(k, add)
            ring_copy(k, j).start()

    for k in range(n):
        own_copy(k, 7).wait()
        sib_copy(k, 7).wait_recv()
        ring_copy(k, 6).wait_recv()
        for copy in loads(k):
            copy.wait()

        def step(at, k=k):
            total = own[k][7, :, at].astype(F32) + sib[k][7, :, at].astype(F32) + rec[k][6, :, at].astype(F32)
            w_at, m_at, v_at = adamw(wv[k][:, at].astype(F32), mv[k][:, at], vv[k][:, at], total.astype(BF16).astype(F32))
            wv[k][:, at] = w_at
            mv[k][:, at] = m_at
            vv[k][:, at] = v_at

        over_columns(k, step)
        gather_copy(k, 0, wv[k]).start()
        twin_copy(k, 0, wv[k]).start()
        for copy in stores(k):
            copy.start()

    @pl.loop(1, 7)
    def _(j):
        for k in range(n):
            gather_copy(k, j - 1, None).wait_recv()
            gather_copy(k, j, None).start()
            twin_copy(k, j, None).start()

    for k in range(n):
        gather_copy(k, 6, None).wait_recv()
        twin_copy(k, 7, None).start()

    @pl.loop(0, 8)
    def _(j):
        for k in range(n):
            sib_copy(k, j).wait_send()
            twin_copy(k, j, None).wait()

    @pl.loop(0, 7)
    def _(j):
        for k in range(n):
            ring_copy(k, j).wait_send()
            gather_copy(k, j, None).wait_send()

    for k in range(n):
        for copy in stores(k):
            copy.wait()


ORDER = ((2, 1), (0, 1), (1, 1), (2, 0), (0, 0), (1, 0))


def ring_step(grads, w, m, v):
    n, shapes = len(ORDER), [one.shape[1:] for one in m]
    dma = pltpu.SemaphoreType.DMA
    scratch = [pltpu.VMEM((blocks, *shapes[name]), BF16) for blocks in (8, 8, 7) for name, _ in ORDER]
    scratch += [pltpu.VMEM(shapes[name], dtype) for dtype in (BF16, F32, F32) for name, _ in ORDER]
    scratch += [dma((n, 8))] * 3 + [dma((n, 7))] * 4 + [dma((n, 8))] * 2 + [dma((n, 3))] * 2
    anywhere = pl.BlockSpec(memory_space=pl.ANY)
    return pl.pallas_call(
        functools.partial(ring_kernel, ORDER, shapes),
        out_shape=[jax.ShapeDtypeStruct(one.shape, one.dtype) for one in (*w, *m, *v)],
        in_specs=[anywhere] * (n + 9),
        out_specs=[anywhere] * 9,
        scratch_shapes=scratch,
        compiler_params=pltpu.CompilerParams(collective_id=0, has_side_effects=True, vmem_limit_bytes=67_000_000),
        name="ring_step",
    )(*grads, *w, *m, *v)


def solution(mesh):
    def body(x, dy, wg, wu, wd, mg, mu, md, vg, vu, vd):
        x, dy = x[0], dy[0]
        a0 = normed(x)
        gate0, up0, act0 = hidden(a0, wg[0], wu[0])
        h1 = x + nn(act0, wd[0]).astype(BF16)
        a1 = normed(h1)
        gate1, up1, act1 = hidden(a1, wg[1], wu[1])
        dact1 = nt(dy, wd[1]).astype(BF16)
        dwd1 = tn(act1, dy).astype(BF16)
        dgate1, dup1 = hidden_back(gate1, up1, dact1)
        dwg1, dwu1 = tn(a1, dgate1).astype(BF16), tn(a1, dup1).astype(BF16)
        da1 = nt(dgate1, wg[1]).astype(BF16) + nt(dup1, wu[1]).astype(BF16)
        dh1 = dy + normed_back(h1, da1)
        dact0 = nt(dh1, wd[0]).astype(BF16)
        dwd0 = tn(act0, dh1).astype(BF16)
        dgate0, dup0 = hidden_back(gate0, up0, dact0)
        dwg0, dwu0 = tn(a0, dgate0).astype(BF16), tn(a0, dup0).astype(BF16)

        def blocks(one):
            return one.reshape(2, 16, -1, one.shape[-1])

        def by_chip(one):
            return one.reshape(8, 2, -1, one.shape[-1])

        grads = [by_chip(one) for one in (dwd1, dwg1, dwu1, dwd0, dwg0, dwu0)]
        new = ring_step(grads, [blocks(one) for one in (wg, wu, wd)], [mg, mu, md], [vg, vu, vd])
        return tuple(one.reshape(2, -1, one.shape[-1]) for one in new[:3]) + tuple(new[3:])

    one, shard = P(("rep", "dp"), None, None), P(None, "dp", None)
    rep = P(None, None, None)
    outs = (P("rep", None, None),) * 3 + (P("rep", "dp", None),) * 6
    return jax.shard_map(body, mesh=mesh, in_specs=(one, one, rep, rep, rep) + (shard,) * 6, out_specs=outs, check_vma=False)
```

```python
import functools

import jax
import jax.numpy as jnp
from jax import lax
from jax.experimental import pallas as pl
from jax.experimental.pallas import tpu as pltpu
from jax.sharding import PartitionSpec as P

F32, BF16 = jnp.float32, jnp.bfloat16


def dot(a, b, contract):
    return lax.dot_general(a, b, (contract, ((), ())), preferred_element_type=F32)


def nn(a, b):
    return dot(a, b, ((1,), (0,)))


def nt(a, b):
    return dot(a, b, ((1,), (1,)))


def adamw(w, m, v, g):
    m = 0.9 * m + 0.1 * g
    v = 0.95 * v + 0.05 * g * g
    step = m * lax.rsqrt(v + 1e-8) + 0.1 * w
    return (w - 0.02 * step).astype(BF16), m, v


def normed(h):
    wide = h.astype(F32)
    scale = lax.rsqrt(jnp.mean(wide**2, -1, keepdims=True) + 1e-6)
    return (wide * scale).astype(BF16)


def normed_back(h, da):
    wide, da = h.astype(F32), da.astype(F32)
    scale = lax.rsqrt(jnp.mean(wide**2, -1, keepdims=True) + 1e-6)
    inner = jnp.mean(wide * da, -1, keepdims=True)
    return (da * scale - wide * (scale * scale * scale * inner)).astype(BF16)


def chain_kernel(tokens, x_ref, dy_ref, *refs):
    weights, refs = refs[:3], refs[3:]
    (a0, act0, dgate0, dup0, a1, act1, dgate1, dup1, dh1), refs = refs[:9], refs[9:]
    held, (gate_keep, up_keep, act_keep, dgate_keep, dup_keep, sem) = refs[:6], refs[6:]
    step = pl.program_id(0)
    wide = 256
    full = gate_keep.shape[1]

    def load(i):
        return pltpu.make_async_copy(weights[i % 3].at[i // 3], held[i], sem.at[i])

    @pl.when(step == 0)
    def _():
        for i in range(6):
            load(i).start()

    def need(i):
        @pl.when(step == 0)
        def _():
            load(i).wait()

    x, dy = x_ref[...], dy_ref[...]
    a = normed(x)
    a0[...] = a.T
    need(0)
    need(1)
    for c in range(0, full, wide):
        at = slice(c, c + wide)
        gate, up = nn(a, held[0][:, at]), nn(a, held[1][:, at])
        act = (jax.nn.silu(gate) * up).astype(BF16)
        gate_keep[:, at] = gate
        up_keep[:, at] = up
        act_keep[:, at] = act
        act0[at, :] = act.T
    need(2)
    h1 = (x.astype(F32) + nn(act_keep[...], held[2][...]).astype(BF16).astype(F32)).astype(BF16)
    a = normed(h1)
    a1[...] = a.T
    for i in (3, 4, 5):
        need(i)
    for c in range(0, full, wide):
        at = slice(c, c + wide)
        gate, up = nn(a, held[3][:, at]), nn(a, held[4][:, at])
        dact = nt(dy, held[5][at, :]).astype(BF16)
        act, dgate, dup = hidden_both(gate, up, dact)
        act1[at, :] = act.T
        dgate_keep[:, at] = dgate
        dup_keep[:, at] = dup
        dgate1[:, at] = dgate
        dup1[:, at] = dup
    da = nt(dgate_keep[...], held[3][...]).astype(BF16).astype(F32) + nt(dup_keep[...], held[4][...]).astype(BF16).astype(F32)
    dh = (dy.astype(F32) + normed_back(h1, da.astype(BF16)).astype(F32)).astype(BF16)
    dh1[...] = dh
    for c in range(0, full, wide):
        at = slice(c, c + wide)
        dact = nt(dh, held[2][at, :]).astype(BF16)
        _, dgate, dup = hidden_both(gate_keep[:, at], up_keep[:, at], dact)
        dgate0[:, at] = dgate
        dup0[:, at] = dup


def hidden_both(gate, up, dact):
    s = jax.nn.sigmoid(gate)
    dact = dact.astype(F32)
    gs = gate * s
    dup = dact * gs
    dgate = dact * up * (s + gs * (1.0 - s))
    return (gs * up).astype(BF16), dgate.astype(BF16), dup.astype(BF16)


def chain(x, dy, wg, wu, wd):
    tokens, d = x.shape
    full, tile = wg.shape[-1], 256
    across = lambda n: pl.BlockSpec((tile, n), lambda i: (i, 0))
    down = lambda n: pl.BlockSpec((n, tile), lambda i: (0, i))
    outs = [(d, True), (full, True), (full, False), (full, False)] * 2 + [(d, False)]
    return pl.pallas_call(
        functools.partial(chain_kernel, tokens),
        grid=(tokens // tile,),
        out_shape=[jax.ShapeDtypeStruct((n, tokens) if t else (tokens, n), BF16) for n, t in outs],
        in_specs=[across(d), across(d)] + [pl.BlockSpec(memory_space=pl.ANY)] * 3,
        out_specs=[down(n) if t else across(n) for n, t in outs],
        scratch_shapes=[pltpu.VMEM(one.shape[1:], BF16) for _ in range(2) for one in (wg, wu, wd)]
        + [pltpu.VMEM((tile, full), F32)] * 2
        + [pltpu.VMEM((tile, full), BF16)] * 3
        + [pltpu.SemaphoreType.DMA((6,))],
        compiler_params=pltpu.CompilerParams(vmem_limit_bytes=67_000_000, dimension_semantics=("arbitrary",)),
        cost_estimate=pl.CostEstimate(flops=18 * tokens * d * full, bytes_accessed=100_000_000, transcendentals=0),
        name="chain",
    )(x, dy, wg, wu, wd)


MESH = pl.DeviceIdType.MESH


def ring_kernel(order, shapes, *refs):
    n = len(order)
    take = iter(refs)
    operands = [(next(take), next(take)) for _ in range(n)]
    w, m, v = ([next(take) for _ in range(3)] for _ in range(3))
    w_new, m_new, v_new = ([next(take) for _ in range(3)] for _ in range(3))
    g, own, sib, rec = ([next(take) for _ in range(n)] for _ in range(4))
    (own_sem, sib_send, sib_recv, rs_send, rs_recv, ag_send, ag_recv, pass_send, pass_recv, load_sem, store_sem) = take

    me = lax.axis_index("dp")
    core, chip = me % 2, me // 2
    far = chip // 4
    place = chip * (1 - far) + far * (11 - chip)
    way = 1 - 2 * core

    def chip_at(p):
        p = (p + 16) % 8
        half = p // 4
        return p * (1 - half) + half * (11 - p)

    after = 2 * chip_at(place + way) + core
    before = 2 * chip_at(place - way) + core
    twin = me + way

    barrier = pltpu.get_barrier_semaphore()
    for other in (after, before, twin):
        pl.semaphore_signal(barrier, inc=1, device_id={"dp": other}, device_id_type=MESH)

    def own_copy(k, j):
        t = chip_at(place - way * (1 + j))
        return pltpu.make_async_copy(g[k].at[2 * t + core], own[k].at[j], own_sem.at[k, j])

    def sib_copy(k, j):
        t = chip_at(place + way * (1 + j))
        return pltpu.make_async_remote_copy(
            g[k].at[2 * t + 1 - core], sib[k].at[j], sib_send.at[k, j], sib_recv.at[k, j], {"dp": twin}, MESH
        )

    def ring_copy(k, j):
        return pltpu.make_async_remote_copy(
            own[k].at[j], rec[k].at[j], rs_send.at[k, j], rs_recv.at[k, j], {"dp": after}, MESH
        )

    def gather_copy(k, j, source=None):
        name, layer = order[k]
        there = w_new[name].at[layer, 2 * chip_at(place - way * j) + core]
        source = there if source is None else source
        return pltpu.make_async_remote_copy(source, there, ag_send.at[k, j], ag_recv.at[k, j], {"dp": after}, MESH)

    def twin_copy(k, j, source=None):
        name, layer = order[k]
        there = w_new[name].at[layer, 2 * chip_at(place - way * j) + core]
        source = there if source is None else source
        return pltpu.make_async_remote_copy(source, there, pass_send.at[k, j], pass_recv.at[k, j], {"dp": twin}, MESH)

    def over_columns(k, body):
        rows, columns = shapes[order[k][0]]
        wide = 256 if columns % 256 == 0 and rows < 100 else 128

        def piece(c, carry):
            body(pl.ds(pl.multiple_of(c * wide, wide), wide))
            return carry

        lax.fori_loop(0, columns // wide, piece, 0)

    def form(k, left, right, pieces, stage, kept_sem, in_sem, out_sem):
        down = order[k][0] == 2
        lhs, rhs = operands[k]
        tiles = g[k].shape[0] // stage.shape[1] if down else g[k].shape[2] // stage.shape[3]

        def get(i, slot):
            if down:
                size = pieces.shape[1]
                source = lhs.at[pl.ds(pl.multiple_of(i * size, size), size), :]
            else:
                size = pieces.shape[2]
                source = rhs.at[:, pl.ds(pl.multiple_of(i * size, size), size)]
            return pltpu.make_async_copy(source, pieces.at[slot], in_sem.at[slot])

        def put(i, slot):
            if down:
                size = stage.shape[1]
                target = g[k].at[pl.ds(pl.multiple_of(i * size, size), size)]
            else:
                size = stage.shape[3]
                target = g[k].at[:, :, pl.ds(pl.multiple_of(i * size, size), size)]
            return pltpu.make_async_copy(stage.at[slot], target, out_sem.at[slot])

        def prefetch():
            get(0, 0).start()
            get(1, 1).start()

        def run():
            @pl.loop(0, tiles)
            def _(i):
                slot = lax.rem(i, 2)
                get(i, slot).wait()
                if down:
                    made = nn(pieces[slot], right[...])
                else:
                    made = nn(left[...], pieces[slot])

                @pl.when(i >= 2)
                def _():
                    put(i, slot).wait()

                stage[slot] = made.reshape(stage.shape[1:]).astype(BF16)
                put(i, slot).start()

                @pl.when(i + 2 < tiles)
                def _():
                    get(i + 2, slot).start()

        def drain():
            put(0, 0).wait()
            put(1, 1).wait()

        return prefetch, run, drain

    def first(k):
        own_copy(k, 0).wait()
        sib_copy(k, 0).wait_recv()

        def add(at):
            own[k][0, :, at] = (own[k][0, :, at].astype(F32) + sib[k][0, :, at].astype(F32)).astype(BF16)

        over_columns(k, add)
        ring_copy(k, 0).start()

    def arrive(k, j):
        own_copy(k, j).wait()
        sib_copy(k, j).wait_recv()
        ring_copy(k, j - 1).wait_recv()

    def total(k, j, at):
        return own[k][j, :, at].astype(F32) + sib[k][j, :, at].astype(F32) + rec[k][j - 1, :, at].astype(F32)

    def onward(k, j):
        arrive(k, j)

        def add(at):
            own[k][j, :, at] = total(k, j, at).astype(BF16)

        over_columns(k, add)
        ring_copy(k, j).start()

    def forming(left, right, wide_in, wide_out, tall_in, tall_out, kept_sem, in_sem, out_sem):
        keep_right = lambda k: pltpu.make_async_copy(operands[k][1], right, kept_sem.at[0])
        keep_left = lambda k: pltpu.make_async_copy(operands[k][0], left, kept_sem.at[1])
        work = []
        for k in range(n):
            kind = int(order[k][0] == 2)
            buffers = (tall_in, tall_out) if kind else (wide_in, wide_out)
            work.append(form(k, left, right, *buffers, kept_sem, in_sem.at[kind], out_sem.at[kind]))
        keep_right(0).start()
        work[0][0]()
        keep_left(1).start()
        keep_right(0).wait()
        for k in range(n):
            work[k][1]()
            if k + 1 < n:
                if k == 0:
                    keep_right(3).start()
                if k == 2:
                    keep_left(4).start()
                work[k + 1][0]()
            work[k][2]()
            if k == 0:
                pl.semaphore_wait(barrier, 3)

            @pl.loop(0, 8)
            def _(j):
                own_copy(k, j).start()
                sib_copy(k, j).start()

            for older in range(k):
                onward(older, k - older)
            first(k)
            if k == 0:
                keep_left(1).wait()
            if k == 2:
                keep_right(3).wait()
            if k == 3:
                keep_left(4).wait()

    dma = pltpu.SemaphoreType.DMA
    pl.run_scoped(
        forming,
        pltpu.VMEM(operands[1][0].shape, BF16),
        pltpu.VMEM(operands[0][1].shape, BF16),
        pltpu.VMEM((2, operands[1][1].shape[0], WIDE), BF16),
        pltpu.VMEM((2, *g[1].shape[:2], WIDE), BF16),
        pltpu.VMEM((2, 2 * g[0].shape[1], operands[0][0].shape[1]), BF16),
        pltpu.VMEM((2, 2, *g[0].shape[1:]), BF16),
        dma((2,)),
        dma((2, 2)),
        dma((2, 2)),
    )

    def closing(*buffers):
        wv, mv, vv = buffers[:n], buffers[n : 2 * n], buffers[2 * n :]

        def loads(k):
            name, layer = order[k]
            return (
                pltpu.make_async_copy(w[name].at[layer, me], wv[k], load_sem.at[k, 0]),
                pltpu.make_async_copy(m[name].at[layer], mv[k], load_sem.at[k, 1]),
                pltpu.make_async_copy(v[name].at[layer], vv[k], load_sem.at[k, 2]),
            )

        def stores(k):
            name, layer = order[k]
            return (
                pltpu.make_async_copy(wv[k], w_new[name].at[layer, me], store_sem.at[k, 0]),
                pltpu.make_async_copy(mv[k], m_new[name].at[layer], store_sem.at[k, 1]),
                pltpu.make_async_copy(vv[k], v_new[name].at[layer], store_sem.at[k, 2]),
            )

        def finish(k):
            arrive(k, 7)
            for copy in loads(k):
                copy.wait()

            def step(at):
                grad = total(k, 7, at).astype(BF16).astype(F32)
                w_at, m_at, v_at = adamw(wv[k][:, at].astype(F32), mv[k][:, at], vv[k][:, at], grad)
                wv[k][:, at] = w_at
                mv[k][:, at] = m_at
                vv[k][:, at] = v_at

            over_columns(k, step)
            gather_copy(k, 0, wv[k]).start()
            twin_copy(k, 0, wv[k]).start()
            for copy in stores(k):
                copy.start()

        for k in range(n):
            for copy in loads(k):
                copy.start()

        @pl.loop(n, n + 14)
        def _(i):
            for k in range(n):
                j = i - k

                @pl.when(j <= 6)
                def _():
                    onward(k, j)

                @pl.when(j == 7)
                def _():
                    finish(k)

                @pl.when((j > 7) & (j < 14))
                def _():
                    gather_copy(k, j - 8).wait_recv()
                    gather_copy(k, j - 7).start()
                    twin_copy(k, j - 7).start()

                @pl.when(j == 14)
                def _():
                    gather_copy(k, 6).wait_recv()
                    twin_copy(k, 7).start()

        @pl.loop(0, 8)
        def _(j):
            for k in range(n):
                sib_copy(k, j).wait_send()
                twin_copy(k, j).wait()

        @pl.loop(0, 7)
        def _(j):
            for k in range(n):
                ring_copy(k, j).wait_send()
                gather_copy(k, j).wait_send()

        for k in range(n):
            for copy in stores(k):
                copy.wait()

    pl.run_scoped(closing, *(pltpu.VMEM(shapes[name], dtype) for dtype in (BF16, F32, F32) for name, _ in order))


ORDER = ((2, 1), (0, 1), (1, 1), (2, 0), (0, 0), (1, 0))
WIDE = 512


def ring_step(operands, w, m, v):
    n, shapes = len(ORDER), [one.shape[1:] for one in m]
    dma = pltpu.SemaphoreType.DMA
    scratch = [pltpu.VMEM((blocks, *shapes[name]), BF16) for blocks in (8, 8, 7) for name, _ in ORDER]
    scratch += [dma((n, 8))] * 3 + [dma((n, 7))] * 4 + [dma((n, 8))] * 2 + [dma((n, 3))] * 2
    anywhere = pl.BlockSpec(memory_space=pl.ANY)
    outs = [jax.ShapeDtypeStruct(one.shape, one.dtype) for one in (*w, *m, *v)]
    outs += [jax.ShapeDtypeStruct((16, *shapes[name]), BF16) for name, _ in ORDER]
    d, full, tokens = 16 * shapes[0][0], shapes[0][1], operands[0][1].shape[0]
    return pl.pallas_call(
        functools.partial(ring_kernel, ORDER, shapes),
        out_shape=outs,
        in_specs=[anywhere] * (2 * n + 9),
        out_specs=[anywhere] * len(outs),
        scratch_shapes=scratch,
        compiler_params=pltpu.CompilerParams(collective_id=0, has_side_effects=True, vmem_limit_bytes=67_000_000),
        cost_estimate=pl.CostEstimate(flops=12 * tokens * d * full, bytes_accessed=200_000_000, transcendentals=0),
        name="ring_step",
    )(*(one for pair in operands for one in pair), *w, *m, *v)[:9]


def solution(mesh):
    def body(x, dy, wg, wu, wd, mg, mu, md, vg, vu, vd):
        x, dy = x[0], dy[0]
        at0, actt0, dgate0, dup0, at1, actt1, dgate1, dup1, dh1 = chain(x, dy, wg, wu, wd)
        def blocks(one):
            return one.reshape(2, 16, -1, one.shape[-1])

        pairs = [(actt1, dy), (at1, dgate1), (at1, dup1), (actt0, dh1), (at0, dgate0), (at0, dup0)]
        new = ring_step(pairs, [blocks(one) for one in (wg, wu, wd)], [mg, mu, md], [vg, vu, vd])
        return tuple(one.reshape(2, -1, one.shape[-1]) for one in new[:3]) + tuple(new[3:])

    one, shard = P(("rep", "dp"), None, None), P(None, "dp", None)
    rep = P(None, None, None)
    outs = (P("rep", None, None),) * 3 + (P("rep", "dp", None),) * 6
    return jax.shard_map(body, mesh=mesh, in_specs=(one, one, rep, rep, rep) + (shard,) * 6, out_specs=outs, check_vma=False)
```

```python
import functools

import jax
import jax.numpy as jnp
from jax import lax
from jax.experimental import pallas as pl
from jax.experimental.pallas import tpu as pltpu
from jax.sharding import PartitionSpec as P

F32, BF16 = jnp.float32, jnp.bfloat16


def dot(a, b, contract):
    return lax.dot_general(a, b, (contract, ((), ())), preferred_element_type=F32)


def nn(a, b):
    return dot(a, b, ((1,), (0,)))


def nt(a, b):
    return dot(a, b, ((1,), (1,)))


def adamw(w, m, v, g):
    m = 0.9 * m + 0.1 * g
    v = 0.95 * v + 0.05 * g * g
    step = m * lax.rsqrt(v + 1e-8) + 0.1 * w
    return (w - 0.02 * step).astype(BF16), m, v


def normed(h):
    wide = h.astype(F32)
    scale = lax.rsqrt(jnp.mean(wide**2, -1, keepdims=True) + 1e-6)
    return (wide * scale).astype(BF16)


def normed_back(h, da):
    wide, da = h.astype(F32), da.astype(F32)
    scale = lax.rsqrt(jnp.mean(wide**2, -1, keepdims=True) + 1e-6)
    inner = jnp.mean(wide * da, -1, keepdims=True)
    return (da * scale - wide * (scale * scale * scale * inner)).astype(BF16)


def chain_kernel(x_ref, dy_ref, *refs):
    weights, refs = refs[:3], refs[3:]
    (a0, act0, gate0, up0, h1_ref, a1, act1, dgate1, dup1), refs = refs[:9], refs[9:]
    held, (act_keep, sem) = refs[:6], refs[6:]
    step = pl.program_id(0)
    wide = 256
    full = act_keep.shape[1]

    def load(i):
        return pltpu.make_async_copy(weights[i % 3].at[i // 3], held[i], sem.at[i])

    @pl.when(step == 0)
    def _():
        for i in range(6):
            load(i).start()

    def need(i):
        @pl.when(step == 0)
        def _():
            load(i).wait()

    x, dy = x_ref[...], dy_ref[...]
    a = normed(x)
    a0[...] = a.T
    need(0)
    need(1)
    for c in range(0, full, wide):
        at = slice(c, c + wide)
        gate, up = nn(a, held[0][:, at]), nn(a, held[1][:, at])
        act = (jax.nn.silu(gate) * up).astype(BF16)
        gate0[:, at] = gate
        up0[:, at] = up
        act_keep[:, at] = act
        act0[at, :] = act.T
    need(2)
    h1 = (x.astype(F32) + nn(act_keep[...], held[2][...]).astype(BF16).astype(F32)).astype(BF16)
    h1_ref[...] = h1
    a = normed(h1)
    a1[...] = a.T
    for i in (3, 4, 5):
        need(i)
    for c in range(0, full, wide):
        at = slice(c, c + wide)
        gate, up = nn(a, held[3][:, at]), nn(a, held[4][:, at])
        dact = nt(dy, held[5][at, :]).astype(BF16)
        act, dgate, dup = hidden_both(gate, up, dact)
        act1[at, :] = act.T
        dgate1[:, at] = dgate
        dup1[:, at] = dup


def hidden_both(gate, up, dact):
    s = jax.nn.sigmoid(gate)
    dact = dact.astype(F32)
    gs = gate * s
    dup = dact * gs
    dgate = dact * up * (s + gs * (1.0 - s))
    return (gs * up).astype(BF16), dgate.astype(BF16), dup.astype(BF16)


TILE = 256


def chain(x, dy, wg, wu, wd):
    tokens, d = x.shape
    full = wg.shape[-1]
    across = lambda n: pl.BlockSpec((TILE, n), lambda i: (i, 0))
    down = lambda n: pl.BlockSpec((n, TILE), lambda i: (0, i))
    outs = [(d, True, BF16), (full, True, BF16), (full, False, F32), (full, False, F32), (d, False, BF16)]
    outs += [(d, True, BF16), (full, True, BF16), (full, False, BF16), (full, False, BF16)]
    return pl.pallas_call(
        chain_kernel,
        grid=(tokens // TILE,),
        out_shape=[jax.ShapeDtypeStruct((n, tokens) if t else (tokens, n), dtype) for n, t, dtype in outs],
        in_specs=[across(d), across(d)] + [pl.BlockSpec(memory_space=pl.ANY)] * 3,
        out_specs=[down(n) if t else across(n) for n, t, _ in outs],
        scratch_shapes=[pltpu.VMEM(one.shape[1:], BF16) for _ in range(2) for one in (wg, wu, wd)]
        + [pltpu.VMEM((TILE, full), BF16), pltpu.SemaphoreType.DMA((6,))],
        compiler_params=pltpu.CompilerParams(vmem_limit_bytes=67_000_000, dimension_semantics=("arbitrary",)),
        cost_estimate=pl.CostEstimate(flops=12 * tokens * d * full, bytes_accessed=130_000_000, transcendentals=0),
        name="chain",
    )(x, dy, wg, wu, wd)


MESH = pl.DeviceIdType.MESH


def ring_kernel(order, shapes, *refs):
    n, half = len(order), len(order) // 2
    take = iter(refs)
    actt1, dy, at1, dgate1, dup1, actt0, at0, gate0, up0, h1 = (next(take) for _ in range(10))
    w, m, v, w_flat = ([next(take) for _ in range(3)] for _ in range(4))
    w_new, m_new, v_new = ([next(take) for _ in range(3)] for _ in range(3))
    g = [next(take) for _ in range(n)]
    dh1, dgate0, dup0 = (next(take) for _ in range(3))
    operands = ((actt1, dy), (at1, dgate1), (at1, dup1), (actt0, dh1), (at0, dgate0), (at0, dup0))
    own, sib, rec, wv, mv, vv = ([next(take) for _ in range(half)] * 2 for _ in range(6))
    (own_sem, sib_send, sib_recv, rs_send, rs_recv, ag_send, ag_recv, pass_send, pass_recv, load_sem, store_sem) = (
        next(take) for _ in range(11)
    )
    ring_free, sib_free, wg1, wu1, wd0, whole_sem = take

    me = lax.axis_index("dp")
    core, chip = me % 2, me // 2
    far = chip // 4
    place = chip * (1 - far) + far * (11 - chip)
    way = 1 - 2 * core

    def chip_at(p):
        p = (p + 16) % 8
        half = p // 4
        return p * (1 - half) + half * (11 - p)

    after = 2 * chip_at(place + way) + core
    before = 2 * chip_at(place - way) + core
    twin = me + way

    barrier = pltpu.get_barrier_semaphore()
    for other in (after, before, twin):
        pl.semaphore_signal(barrier, inc=1, device_id={"dp": other}, device_id_type=MESH)

    def own_copy(k, j):
        t = chip_at(place - way * (1 + j))
        return pltpu.make_async_copy(g[k].at[2 * t + core], own[k].at[j], own_sem.at[k, j])

    def sib_copy(k, j):
        t = chip_at(place + way * (1 + j))
        return pltpu.make_async_remote_copy(
            g[k].at[2 * t + 1 - core], sib[k].at[j], sib_send.at[k, j], sib_recv.at[k, j], {"dp": twin}, MESH
        )

    def ring_copy(k, j):
        return pltpu.make_async_remote_copy(
            own[k].at[j], rec[k].at[j], rs_send.at[k, j], rs_recv.at[k, j], {"dp": after}, MESH
        )

    def gather_copy(k, j, source=None):
        name, layer = order[k]
        there = w_new[name].at[layer, 2 * chip_at(place - way * j) + core]
        source = there if source is None else source
        return pltpu.make_async_remote_copy(source, there, ag_send.at[k, j], ag_recv.at[k, j], {"dp": after}, MESH)

    def twin_copy(k, j, source=None):
        name, layer = order[k]
        there = w_new[name].at[layer, 2 * chip_at(place - way * j) + core]
        source = there if source is None else source
        return pltpu.make_async_remote_copy(source, there, pass_send.at[k, j], pass_recv.at[k, j], {"dp": twin}, MESH)

    def over_columns(k, body):
        rows, columns = shapes[order[k][0]]
        wide = 256 if columns % 256 == 0 and rows < 100 else 128

        def piece(c, carry):
            body(pl.ds(pl.multiple_of(c * wide, wide), wide))
            return carry

        lax.fori_loop(0, columns // wide, piece, 0)

    def loads(k):
        name, layer = order[k]
        return (
            pltpu.make_async_copy(w[name].at[layer, me], wv[k], load_sem.at[k, 0]),
            pltpu.make_async_copy(m[name].at[layer], mv[k], load_sem.at[k, 1]),
            pltpu.make_async_copy(v[name].at[layer], vv[k], load_sem.at[k, 2]),
        )

    def stores(k):
        name, layer = order[k]
        return (
            pltpu.make_async_copy(wv[k], w_new[name].at[layer, me], store_sem.at[k, 0]),
            pltpu.make_async_copy(mv[k], m_new[name].at[layer], store_sem.at[k, 1]),
            pltpu.make_async_copy(vv[k], v_new[name].at[layer], store_sem.at[k, 2]),
        )

    def total(k, j, at):
        return own[k][j, :, at].astype(F32) + sib[k][j, :, at].astype(F32) + rec[k][j - 1, :, at].astype(F32)

    def arrive(k, j):
        own_copy(k, j).wait()
        sib_copy(k, j).wait_recv()
        ring_copy(k, j - 1).wait_recv()

    def first(k):
        own_copy(k, 0).wait()
        sib_copy(k, 0).wait_recv()

        def add(at):
            own[k][0, :, at] = (own[k][0, :, at].astype(F32) + sib[k][0, :, at].astype(F32)).astype(BF16)

        over_columns(k, add)
        if k >= half:
            pl.semaphore_wait(ring_free.at[k - half], 1)
        ring_copy(k, 0).start()

    def onward(k, j):
        arrive(k, j)

        def add(at):
            own[k][j, :, at] = total(k, j, at).astype(BF16)

        over_columns(k, add)
        ring_copy(k, j).start()

    def finish(k):
        arrive(k, 7)
        for copy in loads(k):
            copy.wait()

        def step(at):
            grad = total(k, 7, at).astype(BF16).astype(F32)
            w_at, m_at, v_at = adamw(wv[k][:, at].astype(F32), mv[k][:, at], vv[k][:, at], grad)
            wv[k][:, at] = w_at
            mv[k][:, at] = m_at
            vv[k][:, at] = v_at

        over_columns(k, step)
        if k < half:
            pl.semaphore_signal(ring_free.at[k], inc=1, device_id={"dp": before}, device_id_type=MESH)
            pl.semaphore_signal(sib_free.at[k], inc=1, device_id={"dp": twin}, device_id_type=MESH)
        gather_copy(k, 0, wv[k]).start()
        twin_copy(k, 0, wv[k]).start()
        for copy in stores(k):
            copy.start()

    def hand_on(k, j):
        gather_copy(k, j - 8).wait_recv()
        gather_copy(k, j - 7).start()
        twin_copy(k, j - 7).start()

    def last(k):
        gather_copy(k, 6).wait_recv()
        twin_copy(k, 7).start()

    def service(k, j, least=0):
        for low, high, act in ((0, 0, lambda: first(k)), (1, 6, lambda: onward(k, j)), (7, 7, lambda: finish(k))):
            if high >= least:
                pl.when((j >= low) & (j <= high))(act)
        pl.when((j >= 8) & (j <= 13))(lambda: hand_on(k, j))
        pl.when(j == 14)(lambda: last(k))

    def make_room(k):
        old = k - half

        @pl.loop(0, 7)
        def _(j):
            ring_copy(old, j).wait_send()

        gather_copy(old, 0).wait_send()
        twin_copy(old, 0).wait_send()
        for copy in stores(old):
            copy.wait()
        for copy in loads(k):
            copy.start()
        pl.semaphore_wait(sib_free.at[old], 1)

    def send_off(k, low, high):
        @pl.loop(low, high)
        def _(j):
            own_copy(k, j).start()
            sib_copy(k, j).start()

    def form(k, left, right, pieces, stage, in_sem, out_sem):
        down = order[k][0] == 2
        lhs, rhs = operands[k]
        tiles = 8 if down else g[k].shape[2] // stage.shape[3]

        def target_of(i):
            turn = i // 2
            step = way * (1 + turn) * (2 * (i % 2) - 1) * (1 - i // 7)
            return chip_at(place + step)

        def get(i, slot):
            if down:
                size = pieces.shape[1]
                source = lhs.at[pl.ds(pl.multiple_of(target_of(i) * size, size), size), :]
            else:
                size = pieces.shape[2]
                source = rhs.at[:, pl.ds(pl.multiple_of(i * size, size), size)]
            return pltpu.make_async_copy(source, pieces.at[slot], in_sem.at[slot])

        def put(i, slot):
            if down:
                target = g[k].at[pl.ds(2 * target_of(i), 2)]
            else:
                size = stage.shape[3]
                target = g[k].at[:, :, pl.ds(pl.multiple_of(i * size, size), size)]
            return pltpu.make_async_copy(stage.at[slot], target, out_sem.at[slot])

        def prefetch():
            get(0, 0).start()
            get(1, 1).start()

        def tile(i, settled):
            slot = lax.rem(i, 2)
            get(i, slot).wait()
            made = nn(pieces[slot], right[...]) if down else nn(left[...], pieces[slot])
            if not settled:

                @pl.when(i >= 2)
                def _():
                    put(i, slot).wait()

            stage[slot] = made.reshape(stage.shape[1:]).astype(BF16)
            put(i, slot).start()

            @pl.when(i + 2 < tiles)
            def _():
                get(i + 2, slot).start()

        def settle():
            put(0, 0).wait()
            put(1, 1).wait()

        return prefetch, tile, settle, tiles

    def forming(base, between, left, right, wide_in, wide_out, tall_in, tall_out, kept_sem, in_sem, out_sem):
        keep_right = pltpu.make_async_copy(operands[base][1], right, kept_sem.at[0])
        keep_left = pltpu.make_async_copy(operands[base + 1][0], left, kept_sem.at[1])
        work = []
        for k in range(base, base + half):
            kind = int(order[k][0] == 2)
            buffers = (tall_in, tall_out) if kind else (wide_in, wide_out)
            work.append(form(k, left, right, *buffers, in_sem.at[kind], out_sem.at[kind]))
        keep_right.start()
        work[0][0]()
        keep_left.start()
        work[1][0]()
        keep_right.wait()
        if base:
            make_room(base)
        else:
            for k in range(half):
                for copy in loads(k):
                    copy.start()
            for i in range(3):
                whole(i).start()

        @pl.loop(0, 4)
        def _(turn):
            work[0][1](2 * turn, True)
            work[0][1](2 * turn + 1, True)
            work[0][2]()
            if not base:

                @pl.when(turn == 0)
                def _():
                    pl.semaphore_wait(barrier, 3)

            own_copy(base, turn).start()
            sib_copy(base, turn).start()

            @pl.when(turn == 1)
            def _():
                between(0)
                first(base)

            @pl.when(turn == 3)
            def _():
                between(1)
                onward(base, 1)

        send_off(base, 4, 8)
        keep_left.wait()

        @pl.loop(0, work[1][3])
        def _(i):
            work[1][1](i, False)
            pl.when(i == 1)(lambda: between(2))

            @pl.when(i == 3)
            def _():
                between(3)
                onward(base, 2)

        work[1][2]()
        work[2][0]()
        if base:
            make_room(base + 1)
        send_off(base + 1, 0, 8)

        @pl.loop(0, work[2][3])
        def _(i):
            work[2][1](i, False)

            @pl.when(i == 0)
            def _():
                between(4)
                onward(base, 3)
                first(base + 1)

            pl.when(i == 2)(lambda: between(5))

            @pl.when(i == 3)
            def _():
                between(6)
                onward(base, 4)
                onward(base + 1, 1)

        work[2][2]()
        if base:
            make_room(base + 2)
        send_off(base + 2, 0, 8)

    dma = pltpu.SemaphoreType.DMA
    formers = (
        pltpu.VMEM(at1.shape, BF16),
        pltpu.VMEM(dy.shape, BF16),
        pltpu.VMEM((2, dgate1.shape[0], WIDE), BF16),
        pltpu.VMEM((2, *g[1].shape[:2], WIDE), BF16),
        pltpu.VMEM((2, 2 * g[0].shape[1], actt1.shape[1]), BF16),
        pltpu.VMEM((2, 2, *g[0].shape[1:]), BF16),
        dma((2,)),
        dma((2, 2)),
        dma((2, 2)),
    )

    def round_of(i, base):
        service(base, 5 + i, 5)
        service(base + 1, 2 + i, 2)
        service(base + 2, i)

    def whole(i):
        layer, held = ((1, wg1), (1, wu1), (0, wd0))[i]
        return pltpu.make_async_copy(w_flat[i].at[layer], held, whole_sem.at[i])

    def backward(*buffers):
        arrays, outs = (dgate1, dup1, gate0, up0, h1, dy), (dgate0, dup0, dh1)
        slots, stage, (in_sem, out_sem) = buffers[:6], buffers[6:9], buffers[9:]
        rows = stage[0].shape[0]
        tiles = dy.shape[0] // rows

        def get(i, slot, b):
            source = arrays[b].at[pl.ds(pl.multiple_of(i * rows, rows), rows), :]
            return pltpu.make_async_copy(source, slots[b].at[slot], in_sem.at[slot, b])

        def put(i, b):
            target = outs[b].at[pl.ds(pl.multiple_of(i * rows, rows), rows), :]
            return pltpu.make_async_copy(stage[b], target, out_sem.at[b])

        for i in range(2):
            for b in range(6):
                get(i, i, b).start()
        for i in range(3):
            whole(i).wait()

        @pl.loop(0, tiles)
        def _(i):
            slot = lax.rem(i, 2)
            round_of(i, 0)
            for b in range(6):
                get(i, slot, b).wait()
            da = nt(slots[0][slot], wg1[...]).astype(BF16).astype(F32) + nt(slots[1][slot], wu1[...]).astype(BF16).astype(F32)
            back = normed_back(slots[4][slot], da.astype(BF16)).astype(F32)
            dh = (slots[5][slot].astype(F32) + back).astype(BF16)

            @pl.when(i > 0)
            def _():
                for b in range(3):
                    put(i, b).wait()

            stage[2][...] = dh
            put(i, 2).start()
            wide = 256
            for c in range(0, wd0.shape[0], wide):
                at = slice(c, c + wide)
                dact = nt(dh, wd0[at, :]).astype(BF16)
                _, dgate, dup = hidden_both(slots[2][slot, :, at], slots[3][slot, :, at], dact)
                stage[0][:, at] = dgate
                stage[1][:, at] = dup
            put(i, 0).start()
            put(i, 1).start()

            @pl.when(i + 2 < tiles)
            def _():
                for b in range(6):
                    get(i + 2, slot, b).start()

        for b in range(3):
            put(0, b).wait()

    def leftover(s):
        for k, j in ((0, 13 + s), (1, 10 + s), (2, 8 + s)):
            if j < 14:
                hand_on(k, j)
            elif j == 14:
                last(k)

    pl.run_scoped(functools.partial(forming, 0, lambda s: None), *formers)
    pl.run_scoped(
        backward,
        *(pltpu.VMEM((2, BACK, one.shape[1]), one.dtype) for one in (dgate1, dup1, gate0, up0, h1, dy)),
        *(pltpu.VMEM((BACK, one.shape[1]), BF16) for one in (dgate0, dup0, dh1)),
        dma((2, 6)),
        dma((3,)),
    )
    pl.run_scoped(functools.partial(forming, half, leftover), *formers)

    @pl.loop(0, 15)
    def _(i):
        round_of(i, half)

    @pl.loop(0, 8)
    def _(j):
        for k in range(n):
            sib_copy(k, j).wait_send()
            twin_copy(k, j).wait_recv()

    @pl.loop(0, 7)
    def _(j):
        for k in range(half):
            ring_copy(half + k, j).wait_send()
            gather_copy(half + k, j).wait_send()
            twin_copy(half + k, j).wait_send()

    @pl.loop(1, 7)
    def _(j):
        for k in range(half):
            gather_copy(k, j).wait_send()
            twin_copy(k, j).wait_send()

    for k in range(n):
        twin_copy(k, 7).wait_send()
    for k in range(half, n):
        for copy in stores(k):
            copy.wait()


ORDER = ((2, 1), (0, 1), (1, 1), (2, 0), (0, 0), (1, 0))
WIDE = 512
BACK = 256


def ring_step(operands, w, m, v):
    n, half, shapes = len(ORDER), len(ORDER) // 2, [one.shape[1:] for one in m]
    dma = pltpu.SemaphoreType.DMA
    scratch = [pltpu.VMEM((blocks, *shapes[name]), BF16) for blocks in (8, 8, 7) for name, _ in ORDER[:half]]
    scratch += [pltpu.VMEM(shapes[name], dtype) for dtype in (BF16, F32, F32) for name, _ in ORDER[:half]]
    scratch += [dma((n, 8))] * 3 + [dma((n, 7))] * 4 + [dma((n, 8))] * 2 + [dma((n, 3))] * 2
    scratch += [pltpu.SemaphoreType.REGULAR((half,))] * 2
    scratch += [pltpu.VMEM(one.shape[1:], BF16) for one in w] + [dma((3,))]
    anywhere = pl.BlockSpec(memory_space=pl.ANY)
    by_device = [one.reshape(2, 16, *shape) for one, shape in zip(w, shapes)]
    outs = [jax.ShapeDtypeStruct(one.shape, one.dtype) for one in (*by_device, *m, *v)]
    outs += [jax.ShapeDtypeStruct((16, *shapes[name]), BF16) for name, _ in ORDER]
    d, full, tokens = 16 * shapes[0][0], shapes[0][1], operands[1].shape[0]
    outs += [jax.ShapeDtypeStruct((tokens, width), BF16) for width in (d, full, full)]
    return pl.pallas_call(
        functools.partial(ring_kernel, ORDER, shapes),
        out_shape=outs,
        in_specs=[anywhere] * (len(operands) + 12),
        out_specs=[anywhere] * len(outs),
        scratch_shapes=scratch,
        compiler_params=pltpu.CompilerParams(collective_id=0, has_side_effects=True, vmem_limit_bytes=67_000_000),
        cost_estimate=pl.CostEstimate(flops=18 * tokens * d * full, bytes_accessed=250_000_000, transcendentals=0),
        name="ring_step",
    )(*operands, *by_device, *m, *v, *w)[:9]


def settle_kernel(*refs):
    ins, outs, held, (in_sem, out_sem) = refs[:3], refs[3:6], refs[6:9], refs[9:]
    pieces = [(i, layer, c) for layer in range(2) for c in range(4) for i in range(3)]

    def get(n):
        i, layer, c = pieces[n]
        at = (layer, slice(4 * c, 4 * c + 4))
        return pltpu.make_async_copy(ins[i].at[at], held[i].at[at], in_sem.at[n])

    def put(n):
        i, layer, c = pieces[n]
        at = (layer, slice(4 * c, 4 * c + 4))
        return pltpu.make_async_copy(held[i].at[at], outs[i].at[at], out_sem.at[n])

    for n in range(len(pieces)):
        get(n).start()
    for n in range(len(pieces)):
        get(n).wait()
        put(n).start()
    for n in range(len(pieces)):
        put(n).wait()


def settle(w):
    anywhere = pl.BlockSpec(memory_space=pl.ANY)
    return pl.pallas_call(
        settle_kernel,
        out_shape=[jax.ShapeDtypeStruct(one.shape, one.dtype) for one in w],
        in_specs=[anywhere] * 3,
        out_specs=[anywhere] * 3,
        scratch_shapes=[pltpu.VMEM(one.shape, BF16) for one in w] + [pltpu.SemaphoreType.DMA((24,))] * 2,
        compiler_params=pltpu.CompilerParams(vmem_limit_bytes=67_000_000),
        cost_estimate=pl.CostEstimate(flops=10_000_000, bytes_accessed=55_000_000, transcendentals=0),
        name="settle",
    )(*w)


def solution(mesh):
    def body(x, dy, wg, wu, wd, mg, mu, md, vg, vu, vd):
        x, dy = x[0], dy[0]
        at0, actt0, gate0, up0, h1, at1, actt1, dgate1, dup1 = chain(x, dy, wg, wu, wd)
        operands = (actt1, dy, at1, dgate1, dup1, actt0, at0, gate0, up0, h1)
        new = ring_step(operands, (wg, wu, wd), (mg, mu, md), (vg, vu, vd))
        return tuple(one.reshape(2, -1, one.shape[-1]) for one in settle(new[:3])) + tuple(new[3:])

    one, shard = P(("rep", "dp"), None, None), P(None, "dp", None)
    rep = P(None, None, None)
    outs = (P("rep", None, None),) * 3 + (P("rep", "dp", None),) * 6
    return jax.shard_map(body, mesh=mesh, in_specs=(one, one, rep, rep, rep) + (shard,) * 6, out_specs=outs, check_vma=False)
```
